768 devices in a mesh: dp: 12 (over z), mp: 64 (over y, x, core).
Axes of the slice: x: 4, y: 8, z: 12, core: 2. Of those that a mesh axis runs over, the one named last changes fastest.
Arguments:
- grad_partial: bfloat16 [12, 32, 576, 576], P('dp', None, 'mp'), may hold values from -1.796875 to 1.796875
- owner: int32 [32], replicated, may hold values from 0 to 63, as said below
- offset: int32 [32], replicated, may hold values from 0 to 31, each once
- left_factor: float32 [64, 576, 576], P('mp', None, 'dp'), may hold values from -3 to 3
- right_factor: float32 [64, 576, 576], P('mp', None, 'dp'), may hold values from -3 to 3
- left_basis: bfloat16 [64, 576, 576], P('mp'), may hold values from -0.25 to 0.25
- right_basis: bfloat16 [64, 576, 576], P('mp'), may hold values from -0.25 to 0.25
- momentum: bfloat16 [64, 576, 576], P('mp'), may hold values from -6 to 6
- second_moment: float32 [64, 576, 576], P('mp'), may hold values from 0.2 to 2
Outputs:
- update: bfloat16 [32, 576, 576], P(None, 'mp', 'dp')
- new_left: float32 [64, 576, 576], P('mp', None, 'dp')
- new_right: float32 [64, 576, 576], P('mp', None, 'dp')
- new_momentum: bfloat16 [64, 576, 576], P('mp')
- new_second: float32 [64, 576, 576], P('mp')
The draws below stay inside these ranges and needn't reach their ends.
Inputs may be any that keep to these rules, and one draw needn't show every extreme that they name: No two blocks have the same owner. `offset`: every position belongs to exactly one block.
All inputs are finite; a program needn't handle non-finite values.
Results may differ from the reference program's by a relative error of at most 0.015.
Values may be sent and summed in bfloat16 or wider, within the bound.
A program may use at most 32 MiB of HBM per device.

```python
import math
import jax
import jax.numpy as jnp
from jax import lax

BS = 576
BLOCKS = 32
N_DP = 12
N_MP = 64


def draw_owner(key, part):
    return jax.random.permutation(key, N_MP)[:BLOCKS].astype(jnp.int32)


def steps_of(key, dims, split, least, largest):
    def one(position, parts):
        steps = jax.random.uniform(jax.random.fold_in(jax.random.fold_in(key, 6), position), (parts,), jnp.float32, least / len(split), largest / len(split))
        return jnp.repeat(jnp.exp(steps), dims[position] // parts).reshape((-1,) + (1,) * (len(dims) - position - 1))

    factor_of = one(*split[0])
    for cut in split[1:]:
        factor_of = factor_of * one(*cut)
    return factor_of


def bell_draw(key, extent, width, bound, pieces=(), kind=jnp.bfloat16):
    drawn = jax.random.normal(key, extent, jnp.float32) * width
    if len(pieces) > 0:
        drawn = steps_of(key, extent, pieces, -0.22, 0.18) * drawn
    return jnp.clip(drawn, min=-bound, max=bound).astype(kind)


def setup_inputs(seed: int = 0) -> dict:
    key_of = jax.random.split(jax.random.key(seed), 10)
    grad_partial = bell_draw(key_of[0], (N_DP, BLOCKS, BS, BS), 0.3, 1.796875, ((0, 12), (2, 64)))
    owner = draw_owner(jax.random.fold_in(key_of[9], 71), 0)
    offset = jax.random.permutation(key_of[2], BLOCKS).astype(jnp.int32)
    left_factor = bell_draw(key_of[3], (N_MP, BS, BS), 0.5, 3.0, ((0, 64), (2, 12)), jnp.float32)
    right_factor = bell_draw(key_of[4], (N_MP, BS, BS), 0.5, 3.0, ((0, 64), (2, 12)), jnp.float32)
    left_basis = bell_draw(key_of[5], (N_MP, BS, BS), BS ** -0.5, 0.25, ((0, 64),))
    right_basis = bell_draw(key_of[6], (N_MP, BS, BS), BS ** -0.5, 0.25, ((0, 64),))
    momentum = bell_draw(key_of[7], (N_MP, BS, BS), 1.0, 6.0, ((0, 64),))
    second_moment = jnp.clip(jnp.exp(math.log(2.0) - 2.3025851 * jax.random.uniform(key_of[8], (N_MP, BS, BS), jnp.float32) ** steps_of(key_of[8], (N_MP, BS, BS), ((0, 64),), -0.2, 0.2)), 0.2, 2.0)
    return {"grad_partial": grad_partial, "owner": owner, "offset": offset, "left_factor": left_factor, "right_factor": right_factor, "left_basis": left_basis, "right_basis": right_basis, "momentum": momentum, "second_moment": second_moment}


def contract_first(matrix_a, matrix_b):
    return lax.dot_general(matrix_a, matrix_b, (((0,), (0,)), ((), ())), preferred_element_type=jnp.float32)

def contract_last(matrix_a, matrix_b):
    return lax.dot_general(matrix_a, matrix_b, (((1,), (1,)), ((), ())), preferred_element_type=jnp.float32)

def soap_slot(gradient, left_fac, right_fac, left_basis, right_basis, moment, second, back_rows):
    new_left = 0.95 * left_fac + 0.05 * contract_last(gradient, gradient)
    new_right = 0.95 * right_fac + 0.05 * contract_first(gradient, gradient)
    new_moment = (0.9 * moment.astype(jnp.float32) + 0.1 * gradient.astype(jnp.float32)).astype(jnp.bfloat16)
    turned = contract_first(left_basis, gradient).astype(jnp.bfloat16)
    rotated = jnp.dot(turned, right_basis, preferred_element_type=jnp.float32)
    turned_mom = contract_first(left_basis, new_moment).astype(jnp.bfloat16)
    rotated_mom = jnp.dot(turned_mom, right_basis, preferred_element_type=jnp.float32)
    new_second = 0.95 * second + 0.05 * rotated * rotated
    scaled = (rotated_mom / (jnp.sqrt(new_second) + 1e-08)).astype(jnp.bfloat16)
    unrotated = jnp.dot(left_basis, scaled, preferred_element_type=jnp.float32).astype(jnp.bfloat16)
    return (new_left, new_right, new_moment, new_second, contract_last(unrotated, back_rows))

def reference(grad_partial, owner, offset, left_factor, right_factor, left_basis, right_basis, momentum, second_moment):
    summed = lax.optimization_barrier(jnp.sum(grad_partial, axis=0, dtype=jnp.float32)).astype(jnp.bfloat16)
    slot_ids = jnp.arange(N_MP, dtype=jnp.int32)
    matches = owner[None, :] == slot_ids[:, None]
    occupied = jnp.any(matches, axis=1)
    chosen = jnp.argmax(matches, axis=1).astype(jnp.int32)
    slot_grads = summed[offset[chosen]]

    def per_slot(operands):
        gradient, left_fac, right_fac, lbasis, rbasis, moment, second = operands
        return soap_slot(gradient, left_fac, right_fac, lbasis, rbasis, moment, second, rbasis)
    new_left, new_right, new_moment, new_second, turned_back = lax.map(per_slot, (slot_grads, left_factor, right_factor, left_basis, right_basis, momentum, second_moment))
    keep_mask = occupied[:, None, None]
    new_left = jnp.where(keep_mask, new_left, left_factor)
    new_right = jnp.where(keep_mask, new_right, right_factor)
    new_moment = jnp.where(keep_mask, new_moment, momentum)
    new_second = jnp.where(keep_mask, new_second, second_moment)
    result = turned_back.astype(jnp.bfloat16)
    update = jnp.zeros((BLOCKS, BS, BS), jnp.bfloat16).at[offset].set(result[owner])
    return (update, new_left, new_right, new_moment, new_second)
```

```python
import functools

import jax
import jax.numpy as jnp
from jax import lax
from jax.experimental import pallas as pl
from jax.experimental.pallas import tpu as pltpu
from jax.sharding import PartitionSpec as P

MESH = pl.DeviceIdType.MESH
F32 = jnp.float32
BF16 = jnp.bfloat16

BS = 576
NB = 32
ND = 12
NM = 64
RPD = BS // NM
CPD = BS // ND
LANES = 128
TILES = 5
UNITS = RPD * TILES
PER = 4
HALF = ND // 2

STARTS = [(UNITS * s) // ND for s in range(ND + 1)]
SLOT_OF = {}
for _s in range(ND):
    for _u in range(STARTS[_s], STARTS[_s + 1]):
        SLOT_OF[_u] = _s * PER + _u - STARTS[_s]


def mm(a, b):
    return lax.dot_general(a, b, (((1,), (0,)), ((), ())), preferred_element_type=F32)


def mm_nt(a, b):
    return lax.dot_general(a, b, (((1,), (1,)), ((), ())), preferred_element_type=F32)


def grid2(rows, cols):
    return (
        lax.broadcasted_iota(jnp.int32, (rows, cols), 0),
        lax.broadcasted_iota(jnp.int32, (rows, cols), 1),
    )


def one_hot(mask):
    return jnp.where(mask, 1.0, 0.0).astype(BF16)


def wrap(x, n):
    return lax.rem(x, n)


def kernel(
    gp_hbm, owner_ref, offset_ref, lf_hbm, rf_hbm, lb_hbm, rb_hbm, mom_hbm, sec_hbm,
    upd_hbm, nlf_hbm, nrf_hbm, nmom_hbm, nsec_hbm,
    gp, lf, rf, lb, rb, mom, sec,
    sbuf, land1, out2, land2, gu, out4, land4,
    gn, lbt, lbp, tm, nmom, scaled, nlf, nrf, upd,
    load_sem, store_sem, s1_send, s1_recv, s2_send, s2_recv, s3_send, s3_recv, s4_send, s4_recv,
):
    me_z = lax.axis_index("dp")
    me_m = lax.axis_index("mp")

    loads = [
        pltpu.make_async_copy(src, dst, load_sem.at[i])
        for i, (src, dst) in enumerate(
            ((gp_hbm, gp), (lb_hbm, lb), (rb_hbm, rb), (mom_hbm, mom), (sec_hbm, sec), (lf_hbm, lf), (rf_hbm, rf))
        )
    ]
    for copy in loads:
        copy.start()

    barrier = pltpu.get_barrier_semaphore()

    def greet_z(i, carry):
        pl.semaphore_signal(barrier, inc=1, device_id=(wrap(me_z + i, ND), me_m), device_id_type=MESH)
        return carry

    def greet_m(i, carry):
        pl.semaphore_signal(barrier, inc=1, device_id=(me_z, wrap(me_m + i, NM)), device_id_type=MESH)
        return carry

    lax.fori_loop(1, ND, greet_z, 0)
    lax.fori_loop(1, NM, greet_m, 0)

    loads[0].wait()
    for s in range(ND):
        for k in range(PER):
            u = STARTS[s] + k
            if u < STARTS[s + 1]:
                i, t = u // TILES, u % TILES
                if t < TILES - 1:
                    sbuf[s, k] = gp[i, :, t * LANES : (t + 1) * LANES]
                else:
                    sbuf[s, k] = jnp.zeros((NB, LANES), BF16)
                    sbuf[s, k, :, : BS - t * LANES] = gp[i, :, t * LANES : BS]
            else:
                sbuf[s, k] = jnp.zeros((NB, LANES), BF16)

    pl.semaphore_wait(barrier, ND - 1 + NM - 1)

    def copy1(i):
        to = wrap(me_z + i, ND)
        return pltpu.make_async_remote_copy(
            src_ref=sbuf.at[to], dst_ref=land1.at[me_z], send_sem=s1_send.at[i], recv_sem=s1_recv.at[me_z],
            device_id=(to, me_m), device_id_type=MESH,
        )

    def got1(i):
        frm = wrap(me_z + i, ND)
        return pltpu.make_async_remote_copy(
            src_ref=sbuf.at[frm], dst_ref=land1.at[frm], send_sem=s1_send.at[i], recv_sem=s1_recv.at[frm],
            device_id=(frm, me_m), device_id_type=MESH,
        )

    order = [x for d in range(HALF, 0, -1) for x in ((d, ND - d) if d != HALF else (d,))]
    for i in order:
        copy1(i).start()

    owner = owner_ref[...]
    offset = offset_ref[...]
    occupied = jnp.max(jnp.where(owner == me_m, 1.0, 0.0), axis=1, keepdims=True)
    keep_factor = jnp.where(occupied > 0.5, 0.95, 1.0)
    keep_mom = jnp.where(occupied > 0.5, 0.9, 1.0)
    add_factor = jnp.where(occupied > 0.5, 0.05, 0.0)
    add_mom = jnp.where(occupied > 0.5, 0.1, 0.0)

    row, col = grid2(NM * 8, NB)
    by_owner = one_hot(owner == row // 8)
    row, col = grid2(PER * NB, NB)
    by_offset = one_hot(offset == wrap(row, NB))
    row, col = grid2(NM * 8, PER * NB)
    route = jnp.where(wrap(row, 8) == col // NB, mm_nt(by_owner, by_offset), 0.0).astype(BF16)

    row, col = grid2(BS, BS)
    loads[1].wait()
    lbt[...] = mm_nt(one_hot(row == col), lb[...]).astype(BF16)
    slab = row // NM
    slab = jnp.where(slab < 5, 2 * slab, 2 * slab - 9)
    lbp[...] = mm(one_hot(col == wrap(row, NM) * RPD + slab), lb[...]).astype(BF16)
    for copy in loads[2:]:
        copy.wait()

    total = [sbuf[me_z, k].astype(F32) for k in range(PER)]
    for i in (1, 11, 2, 10, 3, 9, 4, 8, 5, 7, 6):
        got1(i).wait_recv()
        frm = wrap(me_z + i, ND)
        total = [total[k] + land1[frm, k].astype(F32) for k in range(PER)]
    summed = jnp.concatenate(total, axis=0).astype(BF16)

    out2[...] = mm(route, summed).reshape(NM, 8, LANES).astype(BF16)
    land2[me_m] = out2[me_m]

    def send2(i, carry):
        to = wrap(me_m + i, NM)
        pltpu.make_async_remote_copy(
            src_ref=out2.at[to], dst_ref=land2.at[me_m], send_sem=s2_send, recv_sem=s2_recv,
            device_id=(me_z, to), device_id_type=MESH,
        ).start()
        return carry

    lax.fori_loop(1, NM, send2, 0)
    done2 = pltpu.make_async_remote_copy(
        src_ref=out2.at[pl.ds(0, NM - 1)], dst_ref=land2.at[pl.ds(0, NM - 1)], send_sem=s2_send, recv_sem=s2_recv,
        device_id=(me_z, wrap(me_m + 1, NM)), device_id_type=MESH,
    )
    row, col = grid2(PER * NM, NM * 8)
    gather = one_hot(col == wrap(row, NM) * 8 + row // NM)
    done2.wait_recv()
    arrived = land2[...].astype(F32).reshape(NM * 8, LANES).astype(BF16)
    gu[pl.ds(me_z * PER, PER)] = mm(gather, arrived).astype(BF16).reshape(PER, NM, LANES)

    right = (wrap(me_z + 1, ND), me_m)
    left = (wrap(me_z + ND - 1, ND), me_m)

    def hop(way, dist, k):
        origin = wrap(me_z + (ND - dist + 1 if way == 0 else dist - 1), ND)
        slot = gu.at[origin * PER + k]
        return pltpu.make_async_remote_copy(
            src_ref=slot, dst_ref=slot, send_sem=s3_send.at[way, dist - 1, k], recv_sem=s3_recv.at[way, dist - 1, k],
            device_id=right if way == 0 else left, device_id_type=MESH,
        )

    def landed(way, dist, k):
        origin = wrap(me_z + (ND - dist if way == 0 else dist), ND)
        slot = gu.at[origin * PER + k]
        return pltpu.make_async_remote_copy(
            src_ref=slot, dst_ref=slot, send_sem=s3_send.at[way, dist - 1, k], recv_sem=s3_recv.at[way, dist - 1, k],
            device_id=right if way == 0 else left, device_id_type=MESH,
        )

    def goes(way, dist, k):
        return dist < HALF or (dist == HALF and (k < PER // 2) == (way == 0))

    for k in range(PER):
        for way in (0, 1):
            hop(way, 1, k).start()
    for dist in range(1, HALF + 1):
        for k in range(PER):
            for way in (0, 1):
                if goes(way, dist, k):
                    landed(way, dist, k).wait_recv()
                    if goes(way, dist + 1, k):
                        hop(way, dist + 1, k).start()

    row, col = grid2(BS, BS)
    to_rows = one_hot(row == wrap(col, NM) * RPD + col // NM)
    for t in range(TILES):
        tile = jnp.concatenate([gu[SLOT_OF[i * TILES + t]] for i in range(RPD)], axis=0)
        width = min(LANES, BS - t * LANES)
        gn[:, t * LANES : t * LANES + width] = mm(to_rows, tile).astype(BF16)[:, :width]

    nmom[...] = (keep_mom * mom[...].astype(F32) + add_mom * gn[...].astype(F32)).astype(BF16)
    tm[0] = mm(lbt[...], gn[...]).astype(BF16)
    tm[1] = mm(lbt[...], nmom[...]).astype(BF16)
    step = BS // 3
    for part in range(3):
        rows = slice(part * step, (part + 1) * step)
        rotated = mm(tm[0, rows], rb[...])
        rotated_mom = mm(tm[1, rows], rb[...])
        new_second = keep_factor * sec[rows, :] + add_factor * rotated * rotated
        sec[rows, :] = new_second
        scaled[rows, :] = (rotated_mom / (jnp.sqrt(new_second) + 1e-08)).astype(BF16)
    store_second = pltpu.make_async_copy(sec, nsec_hbm, store_sem.at[0])
    store_second.start()
    store_mom = pltpu.make_async_copy(nmom, nmom_hbm, store_sem.at[1])
    store_mom.start()

    unrotated = mm(lbp[...], scaled[...]).astype(BF16)
    back = rb[pl.ds(pl.multiple_of(me_z * CPD, 16), CPD), :]
    zeros = functools.partial(jnp.zeros, dtype=BF16)
    even = mm_nt(unrotated[: 5 * NM], jnp.concatenate([back, zeros((LANES - CPD, BS))], axis=0))
    odd = mm_nt(unrotated[5 * NM :], jnp.concatenate([zeros((CPD, BS)), back, zeros((LANES - 2 * CPD, BS))], axis=0))
    pairs = jnp.concatenate([even[: 4 * NM] + odd, even[4 * NM :]], axis=0).astype(BF16)
    row, col = grid2(NM * 8, 5 * NM)
    spread = one_hot(col == wrap(row, 8) * NM + row // 8)
    out4[...] = mm(spread, pairs).reshape(NM, 8, LANES).astype(BF16)
    land4[me_m] = out4[me_m]

    def send4(i, carry):
        to = wrap(me_m + i, NM)
        pltpu.make_async_remote_copy(
            src_ref=out4.at[to], dst_ref=land4.at[me_m], send_sem=s4_send, recv_sem=s4_recv,
            device_id=(me_z, to), device_id_type=MESH,
        ).start()
        return carry

    lax.fori_loop(1, NM, send4, 0)
    done4 = pltpu.make_async_remote_copy(
        src_ref=out4.at[pl.ds(0, NM - 1)], dst_ref=land4.at[pl.ds(0, NM - 1)], send_sem=s4_send, recv_sem=s4_recv,
        device_id=(me_z, wrap(me_m + 1, NM)), device_id_type=MESH,
    )

    my_rows = gn[pl.ds(pl.multiple_of(me_z * CPD, 16), CPD), :]
    nlf[...] = keep_factor * lf[...] + add_factor * mm_nt(my_rows, gn[...])
    row, col = grid2(CPD, BS)
    my_cols = mm_nt(one_hot(col == row + me_z * CPD), gn[...]).astype(BF16)
    nrf[...] = keep_factor * rf[...] + add_factor * mm(my_cols, gn[...])
    store_left = pltpu.make_async_copy(nlf, nlf_hbm, store_sem.at[2])
    store_left.start()
    store_right = pltpu.make_async_copy(nrf, nrf_hbm, store_sem.at[3])
    store_right.start()

    row, col = grid2(5 * NB, NB)
    at_offset = one_hot(offset == wrap(row, NB))
    row, col = grid2(5 * NB, NM * 8)
    place = jnp.where(row // NB == wrap(col, 8), mm_nt(at_offset, by_owner), 0.0).astype(BF16)

    done4.wait_recv()
    returned = land4[...].astype(F32).reshape(NM * 8, LANES).astype(BF16)
    placed = mm(place, returned).astype(BF16)
    for i in range(RPD):
        pair = placed[(i // 2) * NB : (i // 2 + 1) * NB, :]
        upd[i] = pair[:, (i % 2) * CPD : (i % 2 + 1) * CPD]
    store_update = pltpu.make_async_copy(upd, upd_hbm, store_sem.at[4])
    store_update.start()

    for i in range(1, ND):
        copy1(i).wait_send()
    done2.wait_send()
    for dist in range(1, HALF + 1):
        for k in range(PER):
            for way in (0, 1):
                if goes(way, dist, k):
                    hop(way, dist, k).wait_send()
    done4.wait_send()
    for copy in (store_second, store_mom, store_left, store_right, store_update):
        copy.wait()


def per_device(gp, owner, offset, lf, rf, lb, rb, mom, sec):
    anywhere = pl.BlockSpec(memory_space=pl.ANY)
    whole = pl.BlockSpec(memory_space=pltpu.VMEM)
    dma = pltpu.SemaphoreType.DMA
    outs = pl.pallas_call(
        kernel,
        out_shape=(
            jax.ShapeDtypeStruct((RPD, NB, CPD), BF16),
            jax.ShapeDtypeStruct((CPD, BS), F32),
            jax.ShapeDtypeStruct((CPD, BS), F32),
            jax.ShapeDtypeStruct((BS, BS), BF16),
            jax.ShapeDtypeStruct((BS, BS), F32),
        ),
        in_specs=[anywhere, whole, whole] + [anywhere] * 6,
        out_specs=[anywhere] * 5,
        scratch_shapes=[
            pltpu.VMEM((RPD, NB, BS), BF16),
            pltpu.VMEM((CPD, BS), F32),
            pltpu.VMEM((CPD, BS), F32),
            pltpu.VMEM((BS, BS), BF16),
            pltpu.VMEM((BS, BS), BF16),
            pltpu.VMEM((BS, BS), BF16),
            pltpu.VMEM((BS, BS), F32),
            pltpu.VMEM((ND, PER, NB, LANES), BF16),
            pltpu.VMEM((ND, PER, NB, LANES), BF16),
            pltpu.VMEM((NM, 8, LANES), BF16),
            pltpu.VMEM((NM, 8, LANES), BF16),
            pltpu.VMEM((ND * PER, NM, LANES), BF16),
            pltpu.VMEM((NM, 8, LANES), BF16),
            pltpu.VMEM((NM, 8, LANES), BF16),
            pltpu.VMEM((BS, BS), BF16),
            pltpu.VMEM((BS, BS), BF16),
            pltpu.VMEM((BS, BS), BF16),
            pltpu.VMEM((2, BS, BS), BF16),
            pltpu.VMEM((BS, BS), BF16),
            pltpu.VMEM((BS, BS), BF16),
            pltpu.VMEM((CPD, BS), F32),
            pltpu.VMEM((CPD, BS), F32),
            pltpu.VMEM((RPD, NB, CPD), BF16),
            dma((7,)),
            dma((5,)),
            dma((ND,)),
            dma((ND,)),
            dma,
            dma,
            dma((2, HALF, PER)),
            dma((2, HALF, PER)),
            dma,
            dma,
        ],
        compiler_params=pltpu.CompilerParams(collective_id=0, has_side_effects=True),
    )(
        jnp.transpose(gp[0], (1, 0, 2)),
        owner.reshape(1, NB),
        offset.reshape(1, NB),
        lf[0].T,
        rf[0].T,
        lb[0],
        rb[0],
        mom[0],
        sec[0],
    )
    upd, nlf, nrf, nmom, nsec = outs
    return (jnp.transpose(upd, (1, 0, 2)), nlf.T[None], nrf.T[None], nmom[None], nsec[None])


def solution(mesh):
    block = P("mp", None, None)
    factor = P("mp", None, "dp")
    return jax.shard_map(
        per_device,
        mesh=mesh,
        in_specs=(P("dp", None, "mp", None), P(), P(), factor, factor, block, block, block, block),
        out_specs=(P(None, "mp", "dp"), factor, factor, block, block),
        check_vma=False,
    )
```

```python
import functools

import jax
import jax.numpy as jnp
from jax import lax
from jax.experimental import pallas as pl
from jax.experimental.pallas import tpu as pltpu
from jax.sharding import PartitionSpec as P

MESH = pl.DeviceIdType.MESH
F32 = jnp.float32
BF16 = jnp.bfloat16

BS = 576
NB = 32
ND = 12
NM = 64
RPD = BS // NM
CPD = BS // ND
LANES = 128
FULL = BS // LANES
REST = BS - FULL * LANES
PER = 4
HALF = ND // 2

UNITS = [((i, t),) for i in range(RPD) for t in range(FULL)]
UNITS += [tuple((i, FULL) for i in range(a, min(a + 2, RPD))) for a in range(0, RPD, 2)]
STARTS = [len(UNITS) * s // ND for s in range(ND + 1)]
SLOTS = {}
for _s in range(ND):
    for _u in range(STARTS[_s], STARTS[_s + 1]):
        for _side, _part in enumerate(UNITS[_u]):
            SLOTS[_part] = (_s * PER + _u - STARTS[_s], _side)


def _span(n, d):
    return min(d, n - d)


PEERS = sorted(
    ((dy, dx, dc) for dy in range(8) for dx in range(4) for dc in range(2) if (dy, dx, dc) != (0, 0, 0)),
    key=lambda p: (-_span(8, p[0]) - _span(4, p[1]), p),
)


def mm(a, b):
    return lax.dot_general(a, b, (((1,), (0,)), ((), ())), preferred_element_type=F32)


def mm_nt(a, b):
    return lax.dot_general(a, b, (((1,), (1,)), ((), ())), preferred_element_type=F32)


def grid2(rows, cols):
    return (
        lax.broadcasted_iota(jnp.int32, (rows, cols), 0),
        lax.broadcasted_iota(jnp.int32, (rows, cols), 1),
    )


def one_hot(mask):
    return jnp.where(mask, 1.0, 0.0).astype(BF16)


def wrap(x, n):
    return lax.rem(x, n)


def kernel(
    gp_hbm, owner_hbm, offset_hbm, lf_hbm, rf_hbm, lb_hbm, rb_hbm, mom_hbm, sec_hbm,
    land4, place, nlf, nrf, nmom, sec,
    gp, owner_ref, offset_ref, lf, rf, lb, rb, mom,
    sbuf, land1, summed, out2, land2, gu, out4,
    lbt, lbp, pre, tm, scaled, gn,
    load_sem, s1_send, s1_recv, s2_send, s2_recv, s3_send, s3_recv, s4_send, s4_recv,
):
    me_z = lax.axis_index("dp")
    me_m = lax.axis_index("mp")
    me_y, me_x, me_c = lax.div(me_m, 8), wrap(lax.div(me_m, 2), 4), wrap(me_m, 2)

    def peer(p):
        return wrap(me_y + p[0], 8) * 8 + wrap(me_x + p[1], 4) * 2 + wrap(me_c + p[2], 2)

    def has_four(s):
        n = len(UNITS)
        return lax.div((s + 1) * n, ND) - lax.div(s * n, ND) == PER

    loads = [
        pltpu.make_async_copy(src, dst, load_sem.at[i])
        for i, (src, dst) in enumerate(
            (
                (gp_hbm, gp), (owner_hbm, owner_ref), (offset_hbm, offset_ref), (lb_hbm, lb), (rb_hbm, rb),
                (mom_hbm, mom), (sec_hbm, sec), (lf_hbm, lf), (rf_hbm, rf),
            )
        )
    ]
    for copy in loads:
        copy.start()

    barrier = pltpu.get_barrier_semaphore()

    def greet_z(i, carry):
        pl.semaphore_signal(barrier, inc=1, device_id=(wrap(me_z + i, ND), me_m), device_id_type=MESH)
        return carry

    def greet_m(i, carry):
        pl.semaphore_signal(barrier, inc=1, device_id=(me_z, wrap(me_m + i, NM)), device_id_type=MESH)
        return carry

    lax.fori_loop(1, ND, greet_z, 0)
    lax.fori_loop(1, NM, greet_m, 0)

    loads[0].wait()
    for s in range(ND):
        for u in range(STARTS[s], STARTS[s + 1]):
            parts = [gp[i, :, t * LANES : min(BS, (t + 1) * LANES)] for i, t in UNITS[u]]
            if sum(p.shape[1] for p in parts) < LANES:
                parts.append(jnp.zeros((NB, LANES - parts[0].shape[1]), BF16))
            sbuf[s, u - STARTS[s]] = parts[0] if len(parts) == 1 else jnp.concatenate(parts, axis=1)

    pl.semaphore_wait(barrier, ND - 1 + NM - 1)

    def copy1(i, share, slot, to, last):
        some = pl.ds(PER - 1, 1) if last else pl.ds(0, PER - 1)
        part = 1 if last else 0
        return pltpu.make_async_remote_copy(
            src_ref=sbuf.at[share, some], dst_ref=land1.at[slot, some],
            send_sem=s1_send.at[i, part], recv_sem=s1_recv.at[slot, part],
            device_id=(to, me_m), device_id_type=MESH,
        )

    def out1(i, what):
        to = wrap(me_z + i, ND)
        what(copy1(i, to, me_z, to, False))
        pl.when(has_four(to))(lambda: what(copy1(i, to, me_z, to, True)))

    def in1(i, last):
        frm = wrap(me_z + i, ND)
        return copy1(i, me_z, frm, frm, last)

    def start(copy):
        copy.start()

    def wait_recv(copy):
        copy.wait_recv()

    def wait_send(copy):
        copy.wait_send()

    for i in [x for d in range(HALF, 0, -1) for x in sorted({d, ND - d})]:
        out1(i, start)

    loads[1].wait()
    loads[2].wait()
    owner = owner_ref[...]
    offset = offset_ref[...]
    occupied = jnp.max(jnp.where(owner == me_m, 1.0, 0.0), axis=1, keepdims=True) > 0.5
    keep_factor = jnp.where(occupied, 0.95, 1.0)
    keep_mom = jnp.where(occupied, 0.9, 1.0)
    add_factor = jnp.where(occupied, 0.05, 0.0)
    add_mom = jnp.where(occupied, 0.1, 0.0)

    row, col = grid2(NM * 8, NB)
    by_owner = one_hot(owner == row // 8)
    row, col = grid2(PER * NB, NB)
    by_offset = one_hot(offset == wrap(row, NB))
    row, col = grid2(NM * 8, PER * NB)
    route = jnp.where(wrap(row, 8) == col // NB, mm_nt(by_owner, by_offset), 0.0).astype(BF16)
    row, col = grid2(5 * NB, NB)
    at_offset = one_hot(offset == wrap(row, NB))
    row, col = grid2(5 * NB, NM * 8)
    place[...] = jnp.where(row // NB == wrap(col, 8), mm_nt(at_offset, by_owner), 0.0).astype(BF16)

    row, col = grid2(BS, BS)
    same = one_hot(row == col)
    by_slab = one_hot(col == wrap(row, NM) * RPD + row // NM)
    for copy in loads[3:]:
        copy.wait()
    lbp[...] = mm(by_slab, lb[...]).astype(BF16)
    lbt[...] = mm_nt(same, lb[...]).astype(BF16)
    tm[...] = mm(lbt[...], mom[...]).astype(BF16)
    pre[...] = mm(tm[...], rb[...])
    lbt[...] = mm_nt(same, lbp[...]).astype(BF16)

    total = [sbuf[me_z, k].astype(F32) for k in range(PER - 1)]
    near_first = [x for d in range(1, HALF + 1) for x in sorted({d, ND - d})]
    for i in near_first:
        in1(i, False).wait_recv()
        frm = wrap(me_z + i, ND)
        total = [total[k] + land1[frm, k].astype(F32) for k in range(PER - 1)]
    summed[: (PER - 1) * NB] = jnp.concatenate(total, axis=0).astype(BF16)
    summed[(PER - 1) * NB :] = jnp.zeros((NB, LANES), BF16)

    @pl.when(has_four(me_z))
    def _():
        last = sbuf[me_z, PER - 1].astype(F32)
        for i in near_first:
            in1(i, True).wait_recv()
            last = last + land1[wrap(me_z + i, ND), PER - 1].astype(F32)
        summed[(PER - 1) * NB :] = last.astype(BF16)

    out2[...] = mm(route, summed[...]).reshape(NM, 8, LANES).astype(BF16)

    def spread(src, dst, send_sem, recv_sem):
        for p in PEERS:
            to = peer(p)
            pltpu.make_async_remote_copy(
                src_ref=src.at[to], dst_ref=dst.at[me_m], send_sem=send_sem, recv_sem=recv_sem,
                device_id=(me_z, to), device_id_type=MESH,
            ).start()
        dst[me_m] = src[me_m]
        return pltpu.make_async_remote_copy(
            src_ref=src.at[pl.ds(0, NM - 1)], dst_ref=dst.at[pl.ds(0, NM - 1)], send_sem=send_sem, recv_sem=recv_sem,
            device_id=(me_z, wrap(me_m + 1, NM)), device_id_type=MESH,
        )

    done2 = spread(out2, land2, s2_send, s2_recv)
    row, col = grid2(PER * NM, NM * 8)
    gather = one_hot(col == wrap(row, NM) * 8 + row // NM)
    done2.wait_recv()
    arrived = land2[...].astype(F32).reshape(NM * 8, LANES).astype(BF16)
    gu[pl.ds(me_z * PER, PER)] = mm(gather, arrived).astype(BF16).reshape(PER, NM, LANES)

    def parent(dist):
        return (dist - 1) // 2 * 2

    def hop(way, dist, k, received):
        sign = 1 if way == 0 else -1
        origin = wrap(me_z + ND - sign * (dist if received else parent(dist)), ND)
        slot = gu.at[origin * PER + k]
        copy = pltpu.make_async_remote_copy(
            src_ref=slot, dst_ref=slot, send_sem=s3_send.at[way, dist - 1, k], recv_sem=s3_recv.at[way, dist - 1, k],
            device_id=(wrap(me_z + ND + sign * (dist - parent(dist)), ND), me_m), device_id_type=MESH,
        )
        return copy, origin

    def each(dist, received, what, ks=range(PER)):
        for k in ks:
            for way in (0, 1):
                if dist == HALF and (k < PER // 2) != (way == 0):
                    continue
                copy, origin = hop(way, dist, k, received)
                if k == PER - 1:
                    pl.when(has_four(origin))(functools.partial(what, copy))
                else:
                    what(copy)

    each(2, False, start)
    each(1, False, start)
    for dist in (2, 4):
        for k in range(PER):
            each(dist, True, wait_recv, (k,))
            each(dist + 2, False, start, (k,))
        each(dist + 1, False, start)
    for dist in (1, 3, 5, 6):
        each(dist, True, wait_recv)

    def block():
        tiles = [jnp.concatenate([gu[SLOTS[i, t][0]] for i in range(RPD)], axis=0) for t in range(FULL)]
        rest = []
        for i in range(RPD):
            slot, side = SLOTS[i, FULL]
            rest.append(gu[slot][:, side * REST : (side + 1) * REST])
        return jnp.concatenate(tiles + [jnp.concatenate(rest, axis=0)], axis=1)

    tm[...] = mm(lbt[...], block()).astype(BF16)
    step = BS // 3
    for part in range(3):
        rows = slice(part * step, (part + 1) * step)
        rotated = mm(tm[rows], rb[...])
        new_second = keep_factor * sec[rows, :] + add_factor * rotated * rotated
        sec[rows, :] = new_second
        rotated_mom = 0.9 * pre[rows, :] + 0.1 * rotated
        scaled[rows, :] = (rotated_mom / (jnp.sqrt(new_second) + 1e-08)).astype(BF16)

    unrotated = mm(lbp[...], scaled[...]).astype(BF16)
    back = rb[pl.ds(pl.multiple_of(me_z * CPD, 16), CPD), :]
    zeros = functools.partial(jnp.zeros, dtype=BF16)
    slabs = [unrotated[i * NM : (i + 1) * NM] for i in range(RPD)]
    even = mm_nt(jnp.concatenate(slabs[0::2], axis=0), jnp.concatenate([back, zeros((LANES - CPD, BS))], axis=0))
    odd = mm_nt(
        jnp.concatenate(slabs[1::2], axis=0),
        jnp.concatenate([zeros((CPD, BS)), back, zeros((LANES - 2 * CPD, BS))], axis=0),
    )
    pairs = jnp.concatenate([even[: 4 * NM] + odd, even[4 * NM :]], axis=0).astype(BF16)
    row, col = grid2(NM * 8, 5 * NM)
    out4[...] = mm(one_hot(col == wrap(row, 8) * NM + row // 8), pairs).reshape(NM, 8, LANES).astype(BF16)
    done4 = spread(out4, land4, s4_send, s4_recv)

    row, col = grid2(BS, BS)
    gn[...] = mm(one_hot(row == wrap(col, NM) * RPD + col // NM), block()).astype(BF16)
    nmom[...] = (keep_mom * mom[...].astype(F32) + add_mom * gn[...].astype(F32)).astype(BF16)
    my_rows = gn[pl.ds(pl.multiple_of(me_z * CPD, 16), CPD), :]
    nlf[...] = keep_factor * lf[...] + add_factor * mm_nt(my_rows, gn[...])
    row, col = grid2(CPD, BS)
    my_cols = mm_nt(one_hot(col == row + me_z * CPD), gn[...]).astype(BF16)
    nrf[...] = keep_factor * rf[...] + add_factor * mm(my_cols, gn[...])

    for i in range(1, ND):
        out1(i, wait_send)
    done2.wait_send()
    for dist in range(1, HALF + 1):
        each(dist, False, wait_send)
    done4.wait_send()
    done4.wait_recv()


def finish(
    land4, place, nlf, nrf, nmom, nsec,
    upd_hbm, nlf_hbm, nrf_hbm, nmom_hbm, nsec_hbm, upd, sem,
):
    copies = [
        pltpu.make_async_copy(src, dst, sem.at[i])
        for i, (src, dst) in enumerate(
            ((nsec, nsec_hbm), (nmom, nmom_hbm), (nlf, nlf_hbm), (nrf, nrf_hbm), (upd, upd_hbm))
        )
    ]
    for copy in copies[:4]:
        copy.start()
    returned = land4[...].astype(F32).reshape(NM * 8, LANES).astype(BF16)
    placed = mm(place[...], returned).astype(BF16)
    for i in range(RPD):
        pair = placed[(i // 2) * NB : (i // 2 + 1) * NB, :]
        upd[i] = pair[:, (i % 2) * CPD : (i % 2 + 1) * CPD]
    copies[4].start()
    for copy in copies:
        copy.wait()


def per_device(gp, owner, offset, lf, rf, lb, rb, mom, sec):
    hbm = pl.BlockSpec(memory_space=pltpu.HBM)
    vmem = pl.BlockSpec(memory_space=pltpu.VMEM)
    anywhere = pl.BlockSpec(memory_space=pl.ANY)
    dma = pltpu.SemaphoreType.DMA
    stay = functools.partial(pltpu.with_memory_space_constraint, memory_space=pltpu.HBM)
    inner = pl.pallas_call(
        kernel,
        out_shape=(
            pltpu.VMEM((NM, 8, LANES), BF16),
            pltpu.VMEM((5 * NB, NM * 8), BF16),
            pltpu.VMEM((CPD, BS), F32),
            pltpu.VMEM((CPD, BS), F32),
            pltpu.VMEM((BS, BS), BF16),
            pltpu.VMEM((BS, BS), F32),
        ),
        in_specs=[hbm] * 9,
        out_specs=[vmem] * 6,
        scratch_shapes=[
            pltpu.VMEM((RPD, NB, BS), BF16),
            pltpu.VMEM((1, NB), jnp.int32),
            pltpu.VMEM((1, NB), jnp.int32),
            pltpu.VMEM((CPD, BS), F32),
            pltpu.VMEM((CPD, BS), F32),
            pltpu.VMEM((BS, BS), BF16),
            pltpu.VMEM((BS, BS), BF16),
            pltpu.VMEM((BS, BS), BF16),
            pltpu.VMEM((ND, PER, NB, LANES), BF16),
            pltpu.VMEM((ND, PER, NB, LANES), BF16),
            pltpu.VMEM((PER * NB, LANES), BF16),
            pltpu.VMEM((NM, 8, LANES), BF16),
            pltpu.VMEM((NM, 8, LANES), BF16),
            pltpu.VMEM((ND * PER, NM, LANES), BF16),
            pltpu.VMEM((NM, 8, LANES), BF16),
            pltpu.VMEM((BS, BS), BF16),
            pltpu.VMEM((BS, BS), BF16),
            pltpu.VMEM((BS, BS), F32),
            pltpu.VMEM((BS, BS), BF16),
            pltpu.VMEM((BS, BS), BF16),
            pltpu.VMEM((BS, BS), BF16),
            dma((9,)),
            dma((ND, 2)),
            dma((ND, 2)),
            dma,
            dma,
            dma((2, HALF, PER)),
            dma((2, HALF, PER)),
            dma,
            dma,
        ],
        compiler_params=pltpu.CompilerParams(
            collective_id=0, has_side_effects=True, vmem_limit_bytes=40000 << 10
        ),
    )(
        stay(jnp.transpose(gp[0], (1, 0, 2))),
        stay(owner.reshape(1, NB)),
        stay(offset.reshape(1, NB)),
        stay(lf[0].T),
        stay(rf[0].T),
        stay(lb[0]),
        stay(rb[0]),
        stay(mom[0]),
        stay(sec[0]),
    )
    upd, nlf, nrf, nmom, nsec = pl.pallas_call(
        finish,
        out_shape=(
            jax.ShapeDtypeStruct((RPD, NB, CPD), BF16),
            jax.ShapeDtypeStruct((CPD, BS), F32),
            jax.ShapeDtypeStruct((CPD, BS), F32),
            jax.ShapeDtypeStruct((BS, BS), BF16),
            jax.ShapeDtypeStruct((BS, BS), F32),
        ),
        in_specs=[vmem] * 6,
        out_specs=[anywhere] * 5,
        scratch_shapes=[pltpu.VMEM((RPD, NB, CPD), BF16), dma((5,))],
        compiler_params=pltpu.CompilerParams(vmem_limit_bytes=16 << 20),
    )(*inner)
    return (jnp.transpose(upd, (1, 0, 2)), nlf.T[None], nrf.T[None], nmom[None], nsec[None])


def solution(mesh):
    block = P("mp", None, None)
    factor = P("mp", None, "dp")
    return jax.shard_map(
        per_device,
        mesh=mesh,
        in_specs=(P("dp", None, "mp", None), P(), P(), factor, factor, block, block, block, block),
        out_specs=(P(None, "mp", "dp"), factor, factor, block, block),
        check_vma=False,
    )
```

```python
import functools

import jax
import jax.numpy as jnp
from jax import lax
from jax.experimental import pallas as pl
from jax.experimental.pallas import tpu as pltpu
from jax.sharding import PartitionSpec as P

MESH = pl.DeviceIdType.MESH
F32 = jnp.float32
BF16 = jnp.bfloat16

BS = 576
NB = 32
ND = 12
NM = 64
NY = 8
NQ = NM // NY
AWAY = (0, 2, ND - 2, 1, ND - 1)
RPD = BS // NM
CPD = BS // ND
LANES = 128
FULL = BS // LANES
REST = BS - FULL * LANES
PER = 4
HALF = ND // 2

UNITS = [((i, t),) for i in range(RPD) for t in range(FULL)]
UNITS += [tuple((i, FULL) for i in range(a, min(a + 2, RPD))) for a in range(0, RPD, 2)]
STARTS = [len(UNITS) * s // ND for s in range(ND + 1)]
SLOTS = {}
for _s in range(ND):
    for _u in range(STARTS[_s], STARTS[_s + 1]):
        for _side, _part in enumerate(UNITS[_u]):
            SLOTS[_part] = (_s * PER + _u - STARTS[_s], _side)


def _span(n, d):
    return min(d, n - d)


PEERS = sorted(
    ((dy, dx, dc) for dy in range(8) for dx in range(4) for dc in range(2) if (dy, dx, dc) != (0, 0, 0)),
    key=lambda p: (-_span(8, p[0]) - _span(4, p[1]), p),
)


def mm(a, b):
    return lax.dot_general(a, b, (((1,), (0,)), ((), ())), preferred_element_type=F32)


def mm_nt(a, b):
    return lax.dot_general(a, b, (((1,), (1,)), ((), ())), preferred_element_type=F32)


def grid2(rows, cols):
    return (
        lax.broadcasted_iota(jnp.int32, (rows, cols), 0),
        lax.broadcasted_iota(jnp.int32, (rows, cols), 1),
    )


def one_hot(mask):
    return jnp.where(mask, 1.0, 0.0).astype(BF16)


def wrap(x, n):
    return lax.rem(x, n)


def kernel(
    gp_hbm, owner_hbm, offset_hbm, lf_hbm, rf_hbm, lb_hbm, rb_hbm, mom_hbm, sec_hbm,
    land4, place, nlf, nrf, nmom, sec,
    gp, owner_ref, offset_ref, lf, rf, lb, rb, mom,
    sbuf, land1, agg, summed, out2, land2, out3, land3, gu, out4,
    route, turn, gather, lbt, lbp, pre, tm, scaled, gn,
    load_sem, s1_send, s1_recv, s2_send, s2_recv, s3_send, s3_recv, s4_send, s4_recv, s5_send, s5_recv,
):
    me_z = lax.axis_index("dp")
    me_m = lax.axis_index("mp")
    me_y, me_x, me_c = lax.div(me_m, 8), wrap(lax.div(me_m, 2), 4), wrap(me_m, 2)

    def peer(p):
        return wrap(me_y + p[0], 8) * 8 + wrap(me_x + p[1], 4) * 2 + wrap(me_c + p[2], 2)

    def has_four(s):
        n = len(UNITS)
        return lax.div((s + 1) * n, ND) - lax.div(s * n, ND) == PER

    loads = [
        pltpu.make_async_copy(src, dst, load_sem.at[i])
        for i, (src, dst) in enumerate(
            (
                (gp_hbm, gp), (owner_hbm, owner_ref), (offset_hbm, offset_ref), (lb_hbm, lb), (rb_hbm, rb),
                (mom_hbm, mom), (sec_hbm, sec), (lf_hbm, lf), (rf_hbm, rf),
            )
        )
    ]
    for copy in loads:
        copy.start()

    barrier = pltpu.get_barrier_semaphore()

    me_q = wrap(me_m, NQ)

    def at(dz, dy, dq):
        return (wrap(me_z + dz, ND), wrap(me_y + dy, NY) * NQ + wrap(me_q + dq, NQ))

    def greet(dz, dy, dq):
        pl.semaphore_signal(barrier, inc=1, device_id=at(dz, dy, dq), device_id_type=MESH)

    def greet_y(i, carry):
        greet(0, i, 0)
        return carry

    def greet_q(dz, i, carry):
        greet(dz, 0, i)
        return carry

    for dz in AWAY[1:] + AWAY[:1]:
        lax.fori_loop(0 if dz else 1, NQ, functools.partial(greet_q, dz), 0)
    lax.fori_loop(1, NY, greet_y, 0)

    loads[0].wait()
    for s in range(ND):
        for u in range(STARTS[s], STARTS[s + 1]):
            parts = [gp[i, :, t * LANES : min(BS, (t + 1) * LANES)] for i, t in UNITS[u]]
            if sum(p.shape[1] for p in parts) < LANES:
                parts.append(jnp.zeros((NB, LANES - parts[0].shape[1]), BF16))
            sbuf[s, u - STARTS[s]] = parts[0] if len(parts) == 1 else jnp.concatenate(parts, axis=1)

    pl.semaphore_wait(barrier, len(AWAY) * NQ - 1 + NY - 1)

    def parent(dist):
        return (dist - 1) // 2 * 2

    def hop1(way, dist, part, received):
        sign = 1 if way == 0 else -1
        share = wrap(me_z + ND + sign * (parent(dist) if received else dist), ND)
        if dist == HALF:
            a, n = ((0, 2), None)[part] if way == 0 else ((2, 1), (3, 1))[part]
        else:
            a, n = ((0, PER - 1), (PER - 1, 1))[part]
        some = pl.ds(a, n)
        if dist in (2, 4):
            src = agg.at[way, dist // 2 - 1, some]
        else:
            src = sbuf.at[share, some]
        copy = pltpu.make_async_remote_copy(
            src_ref=src, dst_ref=land1.at[way, dist - 1, some],
            send_sem=s1_send.at[way, dist - 1, part], recv_sem=s1_recv.at[way, dist - 1, part],
            device_id=(wrap(me_z + ND + sign * (dist - parent(dist)), ND), me_m), device_id_type=MESH,
        )
        return copy, share

    def each1(dist, received, what):
        for way in (0, 1):
            what(hop1(way, dist, 0, received)[0])
            if dist == HALF and way == 0:
                continue
            copy, share = hop1(way, dist, 1, received)
            pl.when(has_four(share))(functools.partial(what, copy))

    def start(copy):
        copy.start()

    def wait_recv(copy):
        copy.wait_recv()

    def wait_send(copy):
        copy.wait_send()

    def relay(dist):
        each1(dist + 1, True, wait_recv)
        each1(dist + 2, True, wait_recv)
        for way in (0, 1):
            share = wrap(me_z + ND + (dist if way == 0 else -dist), ND)
            for k in range(PER):
                behind = [dist + 1]
                if dist + 2 < HALF or (k < PER // 2) == (way == 0):
                    behind.append(dist + 2)

                def add(k=k, way=way, share=share, behind=behind):
                    total = sbuf[share, k].astype(F32)
                    for d in behind:
                        total = total + land1[way, d - 1, k].astype(F32)
                    agg[way, dist // 2 - 1, k] = total.astype(BF16)

                if k == PER - 1:
                    pl.when(has_four(share))(add)
                else:
                    add()
        each1(dist, False, start)

    for dist in (6, 5, 3, 1):
        each1(dist, False, start)

    loads[1].wait()
    loads[2].wait()
    owner = owner_ref[...]
    offset = offset_ref[...]
    occupied = jnp.max(jnp.where(owner == me_m, 1.0, 0.0), axis=1, keepdims=True) > 0.5
    keep_factor = jnp.where(occupied, 0.95, 1.0)
    keep_mom = jnp.where(occupied, 0.9, 1.0)
    add_factor = jnp.where(occupied, 0.05, 0.0)
    add_mom = jnp.where(occupied, 0.1, 0.0)

    row, col = grid2(NM * PER, NB)
    by_owner = one_hot(owner == row // PER)
    row, col = grid2(PER * NB, NB)
    by_offset = one_hot(offset == wrap(row, NB))
    row, col = grid2(NM * PER, PER * NB)
    route[...] = jnp.where(wrap(row, PER) == col // NB, mm_nt(by_owner, by_offset), 0.0).astype(BF16)
    row, col = grid2(NM * PER, NM * PER)
    line = NY * PER
    turn[...] = one_hot(col == wrap(row, line) // PER * line + row // line * PER + wrap(row, PER))
    gather[...] = one_hot(col == wrap(row, NQ) * line + wrap(row, NM) // NQ * PER + row // NM)
    row, col = grid2(NM * 8, NB)
    by_owner = one_hot(owner == row // 8)
    row, col = grid2(5 * NB, NB)
    at_offset = one_hot(offset == wrap(row, NB))
    row, col = grid2(5 * NB, NM * 8)
    place[...] = jnp.where(row // NB == wrap(col, 8), mm_nt(at_offset, by_owner), 0.0).astype(BF16)
    row, col = grid2(BS, BS)
    for copy in loads[3:]:
        copy.wait()
    lbp[...] = mm(one_hot(col == wrap(row, NM) * RPD + row // NM), lb[...]).astype(BF16)

    relay(4)

    row, col = grid2(BS, BS)
    same = one_hot(row == col)
    lbt[...] = mm_nt(same, lb[...]).astype(BF16)
    tm[...] = mm(lbt[...], mom[...]).astype(BF16)

    relay(2)

    pre[...] = mm(tm[...], rb[...])
    lbt[...] = mm_nt(same, lbp[...]).astype(BF16)

    each1(1, True, wait_recv)
    each1(2, True, wait_recv)

    def add_up(k):
        total = sbuf[me_z, k].astype(F32)
        for way in (0, 1):
            for d in (1, 2):
                total = total + land1[way, d - 1, k].astype(F32)
        summed[k * NB : (k + 1) * NB] = total.astype(BF16)

    for k in range(PER - 1):
        add_up(k)
    summed[(PER - 1) * NB :] = jnp.zeros((NB, LANES), BF16)
    pl.when(has_four(me_z))(functools.partial(add_up, PER - 1))

    lines = mm(route[...], summed[...]).reshape(NY, line, LANES).astype(BF16)
    out2[...] = lines

    def to_line(dy):
        return pltpu.make_async_remote_copy(
            src_ref=out2.at[wrap(me_y + dy, NY)], dst_ref=land2.at[me_y], send_sem=s2_send, recv_sem=s2_recv,
            device_id=at(0, dy, 0), device_id_type=MESH,
        )

    for dy in (4, 3, 5, 2, 6, 1, 7):
        to_line(dy).start()
    land2[me_y] = out2[me_y]
    done2 = pltpu.make_async_remote_copy(
        src_ref=out2.at[pl.ds(0, NY - 1)], dst_ref=land2.at[pl.ds(0, NY - 1)], send_sem=s2_send, recv_sem=s2_recv,
        device_id=at(0, 1, 0), device_id_type=MESH,
    )
    done2.wait_recv()
    out3[...] = mm(turn[...], land2[...].reshape(NM * PER, LANES)).reshape(NQ, line, LANES).astype(BF16)

    def to_owner(n, dq):
        return pltpu.make_async_remote_copy(
            src_ref=out3.at[wrap(me_q + dq, NQ)], dst_ref=land3.at[n, me_q], send_sem=s5_send.at[n], recv_sem=s5_recv.at[n],
            device_id=at(AWAY[n], 0, dq), device_id_type=MESH,
        )

    for n in (1, 2, 3, 4, 0):
        for dq in (4, 5, 3, 2, 6, 7, 1, 0):
            if n or dq:
                to_owner(n, dq).start()
    land3[0, me_q] = out3[me_q]

    def all_rows(n):
        some = pl.ds(0, NQ if n else NQ - 1)
        return pltpu.make_async_remote_copy(
            src_ref=out3.at[some], dst_ref=land3.at[n, some], send_sem=s5_send.at[n], recv_sem=s5_recv.at[n],
            device_id=at(AWAY[n], 0, 1), device_id_type=MESH,
        )

    def take(n):
        all_rows(n).wait_recv()
        share = mm(gather[...], land3[n].reshape(NM * PER, LANES)).astype(BF16)
        gu[pl.ds(wrap(me_z + ND - AWAY[n], ND) * PER, PER)] = share.reshape(PER, NM, LANES)

    def hop(way, dist, k, received):
        sign = 1 if way == 0 else -1
        origin = wrap(me_z + ND - sign * (dist if received else parent(dist)), ND)
        slot = gu.at[origin * PER + k]
        copy = pltpu.make_async_remote_copy(
            src_ref=slot, dst_ref=slot, send_sem=s3_send.at[way, dist - 1, k], recv_sem=s3_recv.at[way, dist - 1, k],
            device_id=(wrap(me_z + ND + sign * (dist - parent(dist)), ND), me_m), device_id_type=MESH,
        )
        return copy, origin

    def each(dist, received, what, ks=range(PER), ways=(0, 1)):
        for k in ks:
            for way in ways:
                if dist == HALF and (k < PER // 2) != (way == 0):
                    continue
                copy, origin = hop(way, dist, k, received)
                if k == PER - 1:
                    pl.when(has_four(origin))(functools.partial(what, copy))
                else:
                    what(copy)

    take(1)
    each(4, False, start, ways=(0,))
    take(2)
    each(4, False, start, ways=(1,))
    each(3, False, start)
    take(3)
    take(4)
    take(0)
    for k in range(PER):
        each(4, True, wait_recv, (k,))
        each(6, False, start, (k,))
    each(5, False, start)
    for dist in (3, 5, 6):
        each(dist, True, wait_recv)

    def block():
        tiles = [jnp.concatenate([gu[SLOTS[i, t][0]] for i in range(RPD)], axis=0) for t in range(FULL)]
        rest = []
        for i in range(RPD):
            slot, side = SLOTS[i, FULL]
            rest.append(gu[slot][:, side * REST : (side + 1) * REST])
        return jnp.concatenate(tiles + [jnp.concatenate(rest, axis=0)], axis=1)

    tm[...] = mm(lbt[...], block()).astype(BF16)
    step = BS // 3
    for part in range(3):
        rows = slice(part * step, (part + 1) * step)
        rotated = mm(tm[rows], rb[...])
        new_second = keep_factor * sec[rows, :] + add_factor * rotated * rotated
        sec[rows, :] = new_second
        rotated_mom = 0.9 * pre[rows, :] + 0.1 * rotated
        scaled[rows, :] = (rotated_mom / (jnp.sqrt(new_second) + 1e-08)).astype(BF16)

    back = rb[pl.ds(pl.multiple_of(me_z * CPD, 16), CPD), :]
    zeros = functools.partial(jnp.zeros, dtype=BF16)
    twice = jnp.concatenate([back, back, zeros((LANES - 2 * CPD, BS))], axis=0)
    turned_back = mm(lbp[...], mm_nt(scaled[...], twice).astype(BF16))
    slabs = [turned_back[i * NM : (i + 1) * NM] for i in range(RPD)]
    lane = lax.broadcasted_iota(jnp.int32, (NM, LANES), 1)
    pairs = [jnp.where(lane < CPD, slabs[i], slabs[min(i + 1, RPD - 1)]) for i in range(0, RPD, 2)]
    pairs = jnp.concatenate(pairs, axis=0).astype(BF16)
    row, col = grid2(NM * 8, 5 * NM)
    out4[...] = mm(one_hot(col == wrap(row, 8) * NM + row // 8), pairs).reshape(NM, 8, LANES).astype(BF16)
    def spread(src, dst, send_sem, recv_sem):
        for p in PEERS:
            to = peer(p)
            pltpu.make_async_remote_copy(
                src_ref=src.at[to], dst_ref=dst.at[me_m], send_sem=send_sem, recv_sem=recv_sem,
                device_id=(me_z, to), device_id_type=MESH,
            ).start()
        dst[me_m] = src[me_m]
        return pltpu.make_async_remote_copy(
            src_ref=src.at[pl.ds(0, NM - 1)], dst_ref=dst.at[pl.ds(0, NM - 1)], send_sem=send_sem, recv_sem=recv_sem,
            device_id=(me_z, wrap(me_m + 1, NM)), device_id_type=MESH,
        )

    done4 = spread(out4, land4, s4_send, s4_recv)

    row, col = grid2(BS, BS)
    gn[...] = mm(one_hot(row == wrap(col, NM) * RPD + col // NM), block()).astype(BF16)
    nmom[...] = (keep_mom * mom[...].astype(F32) + add_mom * gn[...].astype(F32)).astype(BF16)
    my_rows = gn[pl.ds(pl.multiple_of(me_z * CPD, 16), CPD), :]
    nlf[...] = keep_factor * lf[...] + add_factor * mm_nt(my_rows, gn[...])
    row, col = grid2(CPD, BS)
    my_cols = mm_nt(one_hot(col == row + me_z * CPD), gn[...]).astype(BF16)
    nrf[...] = keep_factor * rf[...] + add_factor * mm(my_cols, gn[...])

    for dist in range(1, HALF + 1):
        each1(dist, False, wait_send)
    done2.wait_send()
    for n in range(len(AWAY)):
        all_rows(n).wait_send()
    for dist in range(3, HALF + 1):
        each(dist, False, wait_send)
    done4.wait_send()
    done4.wait_recv()


def finish(
    land4, place, nlf, nrf, nmom, nsec,
    upd_hbm, nlf_hbm, nrf_hbm, nmom_hbm, nsec_hbm, upd, sem,
):
    copies = [
        pltpu.make_async_copy(src, dst, sem.at[i])
        for i, (src, dst) in enumerate(
            ((nsec, nsec_hbm), (nmom, nmom_hbm), (nlf, nlf_hbm), (nrf, nrf_hbm), (upd, upd_hbm))
        )
    ]
    for copy in copies[:4]:
        copy.start()
    returned = land4[...].astype(F32).reshape(NM * 8, LANES).astype(BF16)
    placed = mm(place[...], returned).astype(BF16)
    for i in range(RPD):
        pair = placed[(i // 2) * NB : (i // 2 + 1) * NB, :]
        upd[i] = pair[:, (i % 2) * CPD : (i % 2 + 1) * CPD]
    copies[4].start()
    for copy in copies:
        copy.wait()


def per_device(gp, owner, offset, lf, rf, lb, rb, mom, sec):
    hbm = pl.BlockSpec(memory_space=pltpu.HBM)
    vmem = pl.BlockSpec(memory_space=pltpu.VMEM)
    anywhere = pl.BlockSpec(memory_space=pl.ANY)
    dma = pltpu.SemaphoreType.DMA
    stay = functools.partial(pltpu.with_memory_space_constraint, memory_space=pltpu.HBM)
    inner = pl.pallas_call(
        kernel,
        out_shape=(
            pltpu.VMEM((NM, 8, LANES), BF16),
            pltpu.VMEM((5 * NB, NM * 8), BF16),
            pltpu.VMEM((CPD, BS), F32),
            pltpu.VMEM((CPD, BS), F32),
            pltpu.VMEM((BS, BS), BF16),
            pltpu.VMEM((BS, BS), F32),
        ),
        in_specs=[hbm] * 9,
        out_specs=[vmem] * 6,
        scratch_shapes=[
            pltpu.VMEM((RPD, NB, BS), BF16),
            pltpu.VMEM((1, NB), jnp.int32),
            pltpu.VMEM((1, NB), jnp.int32),
            pltpu.VMEM((CPD, BS), F32),
            pltpu.VMEM((CPD, BS), F32),
            pltpu.VMEM((BS, BS), BF16),
            pltpu.VMEM((BS, BS), BF16),
            pltpu.VMEM((BS, BS), BF16),
            pltpu.VMEM((ND, PER, NB, LANES), BF16),
            pltpu.VMEM((2, HALF, PER, NB, LANES), BF16),
            pltpu.VMEM((2, 2, PER, NB, LANES), BF16),
            pltpu.VMEM((PER * NB, LANES), BF16),
            pltpu.VMEM((NY, NQ * PER, LANES), BF16),
            pltpu.VMEM((NY, NQ * PER, LANES), BF16),
            pltpu.VMEM((NQ, NY * PER, LANES), BF16),
            pltpu.VMEM((len(AWAY), NQ, NY * PER, LANES), BF16),
            pltpu.VMEM((ND * PER, NM, LANES), BF16),
            pltpu.VMEM((NM, 8, LANES), BF16),
            pltpu.VMEM((NM * PER, PER * NB), BF16),
            pltpu.VMEM((NM * PER, NM * PER), BF16),
            pltpu.VMEM((NM * PER, NM * PER), BF16),
            pltpu.VMEM((BS, BS), BF16),
            pltpu.VMEM((BS, BS), BF16),
            pltpu.VMEM((BS, BS), F32),
            pltpu.VMEM((BS, BS), BF16),
            pltpu.VMEM((BS, BS), BF16),
            pltpu.VMEM((BS, BS), BF16),
            dma((9,)),
            dma((2, HALF, 2)),
            dma((2, HALF, 2)),
            dma,
            dma,
            dma((2, HALF, PER)),
            dma((2, HALF, PER)),
            dma,
            dma,
            dma((len(AWAY),)),
            dma((len(AWAY),)),
        ],
        compiler_params=pltpu.CompilerParams(
            collective_id=0, has_side_effects=True, vmem_limit_bytes=40000 << 10
        ),
    )(
        stay(jnp.transpose(gp[0], (1, 0, 2))),
        stay(owner.reshape(1, NB)),
        stay(offset.reshape(1, NB)),
        stay(lf[0].T),
        stay(rf[0].T),
        stay(lb[0]),
        stay(rb[0]),
        stay(mom[0]),
        stay(sec[0]),
    )
    upd, nlf, nrf, nmom, nsec = pl.pallas_call(
        finish,
        out_shape=(
            jax.ShapeDtypeStruct((RPD, NB, CPD), BF16),
            jax.ShapeDtypeStruct((CPD, BS), F32),
            jax.ShapeDtypeStruct((CPD, BS), F32),
            jax.ShapeDtypeStruct((BS, BS), BF16),
            jax.ShapeDtypeStruct((BS, BS), F32),
        ),
        in_specs=[vmem] * 6,
        out_specs=[anywhere] * 5,
        scratch_shapes=[pltpu.VMEM((RPD, NB, CPD), BF16), dma((5,))],
        compiler_params=pltpu.CompilerParams(vmem_limit_bytes=16 << 20),
    )(*inner)
    return (jnp.transpose(upd, (1, 0, 2)), nlf.T[None], nrf.T[None], nmom[None], nsec[None])


def solution(mesh):
    block = P("mp", None, None)
    factor = P("mp", None, "dp")
    return jax.shard_map(
        per_device,
        mesh=mesh,
        in_specs=(P("dp", None, "mp", None), P(), P(), factor, factor, block, block, block, block),
        out_specs=(P(None, "mp", "dp"), factor, factor, block, block),
        check_vma=False,
    )
```

```python
import functools

import jax
import jax.numpy as jnp
from jax import lax
from jax.experimental import pallas as pl
from jax.experimental.pallas import tpu as pltpu
from jax.sharding import PartitionSpec as P

MESH = pl.DeviceIdType.MESH
F32 = jnp.float32
BF16 = jnp.bfloat16

BS = 576
NB = 32
ND = 12
NM = 64
NY = 8
NQ = NM // NY
AWAY = (0, 2, ND - 2, 1, ND - 1)
RPD = BS // NM
CPD = BS // ND
LANES = 128
FULL = BS // LANES
REST = BS - FULL * LANES
PER = 4
HALF = ND // 2

UNITS = [((i, t),) for i in range(RPD) for t in range(FULL)]
UNITS += [tuple((i, FULL) for i in range(a, min(a + 2, RPD))) for a in range(0, RPD, 2)]
STARTS = [len(UNITS) * s // ND for s in range(ND + 1)]
SLOTS = {}
for _s in range(ND):
    for _u in range(STARTS[_s], STARTS[_s + 1]):
        for _side, _part in enumerate(UNITS[_u]):
            SLOTS[_part] = (_s * PER + _u - STARTS[_s], _side)


def _span(n, d):
    return min(d, n - d)


PEERS = sorted(
    ((dy, dx, dc) for dy in range(8) for dx in range(4) for dc in range(2) if (dy, dx, dc) != (0, 0, 0)),
    key=lambda p: (-_span(8, p[0]) - _span(4, p[1]), p),
)


def mm(a, b):
    return lax.dot_general(a, b, (((1,), (0,)), ((), ())), preferred_element_type=F32)


def mm_nt(a, b):
    return lax.dot_general(a, b, (((1,), (1,)), ((), ())), preferred_element_type=F32)


def grid2(rows, cols):
    return (
        lax.broadcasted_iota(jnp.int32, (rows, 1), 0),
        lax.broadcasted_iota(jnp.int32, (1, cols), 1),
    )


def one_hot(mask):
    return jnp.where(mask, 1.0, 0.0).astype(BF16)


def wrap(x, n):
    return lax.rem(x, n)


def roll(x, lanes):
    return pltpu.roll(x, lanes % LANES, 1) if lanes % LANES else x


def pieces(q):
    where = []
    for i in range(RPD):
        lo, hi = max(i * CPD, q * LANES), min((i + 1) * CPD, (q + 1) * LANES)
        if lo < hi:
            where.append((i, lo - q * LANES, hi - q * LANES))
    return where


def kernel(
    gp_hbm, owner_hbm, offset_hbm, lf_hbm, rf_hbm, lb_hbm, rb_hbm, mom_hbm, sec_hbm,
    land4, place, nlf, nrf, nmom, sec,
    gp, owner_ref, offset_ref, lf, rf, lb, rb, mom,
    sbuf, land1, agg, summed, out2, land2, out3, land3, gu, out4,
    route, turn, gather, lbt, lbp, pre, tm, scaled, gn,
    load_sem, s1_send, s1_recv, s2_send, s2_recv, s3_send, s3_recv, s4_send, s4_recv, s5_send, s5_recv,
):
    me_z = lax.axis_index("dp")
    me_m = lax.axis_index("mp")
    me_y, me_x, me_c = lax.div(me_m, 8), wrap(lax.div(me_m, 2), 4), wrap(me_m, 2)

    me_q = wrap(me_m, NQ)
    zs = [wrap(me_z + d, ND) for d in range(ND)]
    ys = [wrap(me_y + d, NY) for d in range(NY)]
    rows_y = [y * NQ for y in ys]
    qs = [wrap(me_q + d, NQ) for d in range(NQ)]
    xs = [wrap(me_x + d, 4) * 2 for d in range(4)]
    cs = [wrap(me_c + d, 2) for d in range(2)]

    def peer(p):
        return rows_y[p[0]] + xs[p[1]] + cs[p[2]]

    ends = [lax.div((z + 1) * len(UNITS), ND) - lax.div(z * len(UNITS), ND) for z in zs]
    fours = [n == PER for n in ends]

    def has_four(off):
        return fours[off % ND]

    loads = [
        pltpu.make_async_copy(src, dst, load_sem.at[i])
        for i, (src, dst) in enumerate(
            (
                (gp_hbm, gp), (owner_hbm, owner_ref), (offset_hbm, offset_ref), (lb_hbm, lb), (rb_hbm, rb),
                (mom_hbm, mom), (sec_hbm, sec), (lf_hbm, lf), (rf_hbm, rf),
            )
        )
    ]
    loads[0].start()

    barrier = pltpu.get_barrier_semaphore()

    def at(dz, dy, dq):
        return (zs[dz % ND], rows_y[dy] + qs[dq])

    def greet(dz, dy, dq):
        pl.semaphore_signal(barrier, inc=1, device_id=at(dz, dy, dq), device_id_type=MESH)

    for dy in (4, 3, 5, 2, 6, 1, 7):
        greet(0, dy, 0)
    for dz in AWAY[1:] + AWAY[:1]:
        for dq in (4, 5, 3, 2, 6, 7, 1, 0):
            if dz or dq:
                greet(dz, 0, dq)

    loads[0].wait()
    for s in range(ND):
        for u in range(STARTS[s], STARTS[s + 1]):
            parts = [gp[i, :, t * LANES : min(BS, (t + 1) * LANES)] for i, t in UNITS[u]]
            if sum(p.shape[1] for p in parts) < LANES:
                parts.append(jnp.zeros((NB, LANES - parts[0].shape[1]), BF16))
            sbuf[s, u - STARTS[s]] = parts[0] if len(parts) == 1 else jnp.concatenate(parts, axis=1)

    for copy in loads[1:]:
        copy.start()
    pl.semaphore_wait(barrier, len(AWAY) * NQ - 1 + NY - 1)

    def parent(dist):
        return (dist - 1) // 2 * 2

    def hop1(way, dist, part, received):
        sign = 1 if way == 0 else -1
        off = sign * (parent(dist) if received else dist)
        share = zs[off % ND]
        if dist == HALF:
            a, n = ((0, 2), None)[part] if way == 0 else ((2, 1), (3, 1))[part]
        else:
            a, n = ((0, PER - 1), (PER - 1, 1))[part]
        some = pl.ds(a, n)
        if dist in (2, 4):
            src = agg.at[way, dist // 2 - 1, some]
        else:
            src = sbuf.at[share, some]
        copy = pltpu.make_async_remote_copy(
            src_ref=src, dst_ref=land1.at[way, dist - 1, some],
            send_sem=s1_send.at[way, dist - 1, part], recv_sem=s1_recv.at[way, dist - 1, part],
            device_id=(zs[sign * (dist - parent(dist)) % ND], me_m), device_id_type=MESH,
        )
        return copy, off

    def each1(dist, received, what):
        for way in (0, 1):
            what(hop1(way, dist, 0, received)[0])
            if dist == HALF and way == 0:
                continue
            copy, off = hop1(way, dist, 1, received)
            pl.when(has_four(off))(functools.partial(what, copy))

    def start(copy):
        copy.start()

    def wait_recv(copy):
        copy.wait_recv()

    def wait_send(copy):
        copy.wait_send()

    def relay(dist):
        each1(dist + 1, True, wait_recv)
        each1(dist + 2, True, wait_recv)
        for way in (0, 1):
            off = dist if way == 0 else -dist
            share = zs[off % ND]
            for k in range(PER):
                behind = [dist + 1]
                if dist + 2 < HALF or (k < PER // 2) == (way == 0):
                    behind.append(dist + 2)

                def add(k=k, way=way, share=share, behind=behind):
                    total = sbuf[share, k].astype(F32)
                    for d in behind:
                        total = total + land1[way, d - 1, k].astype(F32)
                    agg[way, dist // 2 - 1, k] = total.astype(BF16)

                if k == PER - 1:
                    pl.when(has_four(off))(add)
                else:
                    add()
        each1(dist, False, start)

    for dist in (6, 5, 3, 1):
        each1(dist, False, start)

    loads[1].wait()
    loads[2].wait()
    owner = owner_ref[...]
    offset = offset_ref[...]
    occupied = jnp.max(jnp.where(owner == me_m, 1.0, 0.0), axis=1, keepdims=True) > 0.5
    keep_factor = jnp.where(occupied, 0.95, 1.0)
    keep_mom = jnp.where(occupied, 0.9, 1.0)
    add_factor = jnp.where(occupied, 0.05, 0.0)
    add_mom = jnp.where(occupied, 0.1, 0.0)

    row, col = grid2(NM * PER, NB)
    by_owner = one_hot(owner == row // PER)
    row, col = grid2(PER * NB, NB)
    by_offset = one_hot(offset == wrap(row, NB))
    row, col = grid2(NM * PER, PER * NB)
    route[...] = jnp.where(wrap(row, PER) == col // NB, mm_nt(by_owner, by_offset), 0.0).astype(BF16)
    row, col = grid2(BS, BS)
    for copy in loads[3:]:
        copy.wait()
    lbp[...] = mm(one_hot(col == wrap(row, NM) * RPD + row // NM), lb[...]).astype(BF16)

    relay(4)

    row, col = grid2(BS, BS)
    same = one_hot(row == col)
    lbt[...] = mm_nt(same, lb[...]).astype(BF16)
    tm[...] = mm(lbt[...], mom[...]).astype(BF16)

    relay(2)

    pre[...] = mm(tm[...], rb[...])
    lbt[...] = mm_nt(same, lbp[...]).astype(BF16)

    each1(1, True, wait_recv)
    each1(2, True, wait_recv)

    def add_up(k):
        total = sbuf[me_z, k].astype(F32)
        for way in (0, 1):
            for d in (1, 2):
                total = total + land1[way, d - 1, k].astype(F32)
        summed[k * NB : (k + 1) * NB] = total.astype(BF16)

    for k in range(PER - 1):
        add_up(k)
    summed[(PER - 1) * NB :] = jnp.zeros((NB, LANES), BF16)
    pl.when(has_four(0))(functools.partial(add_up, PER - 1))

    line = NY * PER
    lines = mm(route[...], summed[...]).reshape(NY, line, LANES).astype(BF16)
    out2[...] = lines

    def to_line(dy):
        return pltpu.make_async_remote_copy(
            src_ref=out2.at[ys[dy]], dst_ref=land2.at[me_y], send_sem=s2_send, recv_sem=s2_recv,
            device_id=at(0, dy, 0), device_id_type=MESH,
        )

    for dy in (4, 3, 5, 2, 6, 1, 7):
        to_line(dy).start()
    land2[me_y] = out2[me_y]
    done2 = pltpu.make_async_remote_copy(
        src_ref=out2.at[pl.ds(0, NY - 1)], dst_ref=land2.at[pl.ds(0, NY - 1)], send_sem=s2_send, recv_sem=s2_recv,
        device_id=at(0, 1, 0), device_id_type=MESH,
    )
    row, col = grid2(NM * PER, NM * PER)
    turn[...] = one_hot(col == wrap(row, line) // PER * line + row // line * PER + wrap(row, PER))
    gather[...] = one_hot(col == wrap(row, NQ) * line + wrap(row, NM) // NQ * PER + row // NM)
    done2.wait_recv()
    out3[...] = mm(turn[...], land2[...].reshape(NM * PER, LANES)).reshape(NQ, line, LANES).astype(BF16)

    def to_owner(n, dq):
        return pltpu.make_async_remote_copy(
            src_ref=out3.at[qs[dq]], dst_ref=land3.at[n, me_q], send_sem=s5_send.at[n], recv_sem=s5_recv.at[n],
            device_id=at(AWAY[n], 0, dq), device_id_type=MESH,
        )

    for n in (1, 2, 3, 4, 0):
        for dq in (4, 5, 3, 2, 6, 7, 1, 0):
            if n or dq:
                to_owner(n, dq).start()
    land3[0, me_q] = out3[me_q]

    def all_rows(n):
        some = pl.ds(0, NQ if n else NQ - 1)
        return pltpu.make_async_remote_copy(
            src_ref=out3.at[some], dst_ref=land3.at[n, some], send_sem=s5_send.at[n], recv_sem=s5_recv.at[n],
            device_id=at(AWAY[n], 0, 1), device_id_type=MESH,
        )

    def take(n):
        all_rows(n).wait_recv()
        share = mm(gather[...], land3[n].reshape(NM * PER, LANES)).astype(BF16)
        gu[pl.ds(zs[-AWAY[n] % ND] * PER, PER)] = share.reshape(PER, NM, LANES)

    def hop(way, dist, k, received):
        sign = 1 if way == 0 else -1
        off = -sign * (dist if received else parent(dist))
        slot = gu.at[zs[off % ND] * PER + k]
        copy = pltpu.make_async_remote_copy(
            src_ref=slot, dst_ref=slot, send_sem=s3_send.at[way, dist - 1, k], recv_sem=s3_recv.at[way, dist - 1, k],
            device_id=(zs[sign * (dist - parent(dist)) % ND], me_m), device_id_type=MESH,
        )
        return copy, off

    def each(dist, received, what, ks=range(PER), ways=(0, 1)):
        for k in ks:
            for way in ways:
                if dist == HALF and (k < PER // 2) != (way == 0):
                    continue
                copy, off = hop(way, dist, k, received)
                if k == PER - 1:
                    pl.when(has_four(off))(functools.partial(what, copy))
                else:
                    what(copy)

    take(1)
    each(4, False, start, ways=(0,))
    take(2)
    each(4, False, start, ways=(1,))
    each(3, False, start)
    take(3)
    take(4)
    take(0)
    for k in range(PER):
        each(4, True, wait_recv, (k,))
        each(6, False, start, (k,))
    each(5, False, start)
    for dist in (3, 5, 6):
        each(dist, True, wait_recv)

    def block():
        tiles = [jnp.concatenate([gu[SLOTS[i, t][0]] for i in range(RPD)], axis=0) for t in range(FULL)]
        rest = []
        for i in range(RPD):
            slot, side = SLOTS[i, FULL]
            rest.append(gu[slot][:, side * REST : (side + 1) * REST])
        return jnp.concatenate(tiles + [jnp.concatenate(rest, axis=0)], axis=1)

    tm[...] = mm(lbt[...], block()).astype(BF16)
    step = BS // 3
    for part in range(3):
        rows = slice(part * step, (part + 1) * step)
        rotated = mm(tm[rows], rb[...])
        new_second = keep_factor * sec[rows, :] + add_factor * rotated * rotated
        sec[rows, :] = new_second
        rotated_mom = 0.9 * pre[rows, :] + 0.1 * rotated
        scaled[rows, :] = (rotated_mom / (jnp.sqrt(new_second) + 1e-08)).astype(BF16)

    back = rb[pl.ds(pl.multiple_of(me_z * CPD, 16), CPD), :]
    zeros = functools.partial(jnp.zeros, dtype=BF16)
    wide = jnp.concatenate([back, zeros((LANES - CPD, BS))], axis=0)
    turned_back = mm(lbp[...], mm_nt(scaled[...], wide).astype(BF16))
    lane = lax.broadcasted_iota(jnp.int32, (1, LANES), 1)
    packed = []
    for q in range(PER):
        line_q = jnp.zeros((NM, LANES), F32)
        for i, lo, hi in pieces(q):
            moved = roll(turned_back[i * NM : (i + 1) * NM], i * CPD - q * LANES)
            line_q = jnp.where((lane >= lo) & (lane < hi), moved, line_q)
        packed.append(line_q)
    packed = jnp.concatenate(packed, axis=0).astype(BF16)
    row, col = grid2(NM * PER, NM * PER)
    by_holder = one_hot(col == wrap(row, PER) * NM + row // PER)
    out4[...] = mm(by_holder, packed).reshape(NM, PER, LANES).astype(BF16)

    def spread(src, dst, send_sem, recv_sem):
        for p in PEERS:
            to = peer(p)
            pltpu.make_async_remote_copy(
                src_ref=src.at[to], dst_ref=dst.at[me_m], send_sem=send_sem, recv_sem=recv_sem,
                device_id=(me_z, to), device_id_type=MESH,
            ).start()
        dst[me_m] = src[me_m]
        return pltpu.make_async_remote_copy(
            src_ref=src.at[pl.ds(0, NM - 1)], dst_ref=dst.at[pl.ds(0, NM - 1)], send_sem=send_sem, recv_sem=recv_sem,
            device_id=(me_z, peer((0, 0, 1))), device_id_type=MESH,
        )

    done4 = spread(out4, land4, s4_send, s4_recv)

    row, col = grid2(NM * PER, NB)
    by_owner = one_hot(owner == row // PER)
    row, col = grid2(PER * NB, NB)
    at_offset = one_hot(offset == wrap(row, NB))
    row, col = grid2(PER * NB, NM * PER)
    place[...] = jnp.where(row // NB == wrap(col, PER), mm_nt(at_offset, by_owner), 0.0).astype(BF16)

    row, col = grid2(BS, BS)
    gn[...] = mm(one_hot(row == wrap(col, NM) * RPD + col // NM), block()).astype(BF16)
    nmom[...] = (keep_mom * mom[...].astype(F32) + add_mom * gn[...].astype(F32)).astype(BF16)
    my_rows = gn[pl.ds(pl.multiple_of(me_z * CPD, 16), CPD), :]
    nlf[...] = keep_factor * lf[...] + add_factor * mm_nt(my_rows, gn[...])
    row, col = grid2(CPD, BS)
    my_cols = mm_nt(one_hot(col == row + me_z * CPD), gn[...]).astype(BF16)
    nrf[...] = keep_factor * rf[...] + add_factor * mm(my_cols, gn[...])

    for dist in range(1, HALF + 1):
        each1(dist, False, wait_send)
    done2.wait_send()
    for n in range(len(AWAY)):
        all_rows(n).wait_send()
    for dist in (3, 4, 5, 6):
        each(dist, False, wait_send)
    done4.wait_send()
    done4.wait_recv()


def finish(
    land4, place, nlf, nrf, nmom, nsec,
    upd_hbm, nlf_hbm, nrf_hbm, nmom_hbm, nsec_hbm, upd, sem,
):
    copies = [
        pltpu.make_async_copy(src, dst, sem.at[i])
        for i, (src, dst) in enumerate(
            ((nsec, nsec_hbm), (nmom, nmom_hbm), (nlf, nlf_hbm), (nrf, nrf_hbm), (upd, upd_hbm))
        )
    ]
    for copy in copies[:4]:
        copy.start()
    returned = land4[...].astype(F32).reshape(NM * PER, LANES).astype(BF16)
    placed = mm(place[...], returned)
    lane = lax.broadcasted_iota(jnp.int32, (1, LANES), 1)
    for i in range(RPD):
        mine = jnp.zeros((NB, LANES), F32)
        for q in range(PER):
            for other, lo, hi in pieces(q):
                if other == i:
                    moved = roll(placed[q * NB : (q + 1) * NB], q * LANES - i * CPD)
                    mine = jnp.where(lane >= q * LANES + lo - i * CPD, moved, mine)
        upd[i] = mine[:, :CPD].astype(BF16)
    copies[4].start()
    for copy in copies:
        copy.wait()


def per_device(gp, owner, offset, lf, rf, lb, rb, mom, sec):
    hbm = pl.BlockSpec(memory_space=pltpu.HBM)
    vmem = pl.BlockSpec(memory_space=pltpu.VMEM)
    anywhere = pl.BlockSpec(memory_space=pl.ANY)
    dma = pltpu.SemaphoreType.DMA
    stay = functools.partial(pltpu.with_memory_space_constraint, memory_space=pltpu.HBM)
    inner = pl.pallas_call(
        kernel,
        out_shape=(
            pltpu.VMEM((NM, PER, LANES), BF16),
            pltpu.VMEM((PER * NB, NM * PER), BF16),
            pltpu.VMEM((CPD, BS), F32),
            pltpu.VMEM((CPD, BS), F32),
            pltpu.VMEM((BS, BS), BF16),
            pltpu.VMEM((BS, BS), F32),
        ),
        in_specs=[hbm] * 9,
        out_specs=[vmem] * 6,
        scratch_shapes=[
            pltpu.VMEM((RPD, NB, BS), BF16),
            pltpu.VMEM((1, NB), jnp.int32),
            pltpu.VMEM((1, NB), jnp.int32),
            pltpu.VMEM((CPD, BS), F32),
            pltpu.VMEM((CPD, BS), F32),
            pltpu.VMEM((BS, BS), BF16),
            pltpu.VMEM((BS, BS), BF16),
            pltpu.VMEM((BS, BS), BF16),
            pltpu.VMEM((ND, PER, NB, LANES), BF16),
            pltpu.VMEM((2, HALF, PER, NB, LANES), BF16),
            pltpu.VMEM((2, 2, PER, NB, LANES), BF16),
            pltpu.VMEM((PER * NB, LANES), BF16),
            pltpu.VMEM((NY, NQ * PER, LANES), BF16),
            pltpu.VMEM((NY, NQ * PER, LANES), BF16),
            pltpu.VMEM((NQ, NY * PER, LANES), BF16),
            pltpu.VMEM((len(AWAY), NQ, NY * PER, LANES), BF16),
            pltpu.VMEM((ND * PER, NM, LANES), BF16),
            pltpu.VMEM((NM, PER, LANES), BF16),
            pltpu.VMEM((NM * PER, PER * NB), BF16),
            pltpu.VMEM((NM * PER, NM * PER), BF16),
            pltpu.VMEM((NM * PER, NM * PER), BF16),
            pltpu.VMEM((BS, BS), BF16),
            pltpu.VMEM((BS, BS), BF16),
            pltpu.VMEM((BS, BS), F32),
            pltpu.VMEM((BS, BS), BF16),
            pltpu.VMEM((BS, BS), BF16),
            pltpu.VMEM((BS, BS), BF16),
            dma((9,)),
            dma((2, HALF, 2)),
            dma((2, HALF, 2)),
            dma,
            dma,
            dma((2, HALF, PER)),
            dma((2, HALF, PER)),
            dma,
            dma,
            dma((len(AWAY),)),
            dma((len(AWAY),)),
        ],
        compiler_params=pltpu.CompilerParams(
            collective_id=0, has_side_effects=True, vmem_limit_bytes=40000 << 10
        ),
    )(
        stay(jnp.transpose(gp[0], (1, 0, 2))),
        stay(owner.reshape(1, NB)),
        stay(offset.reshape(1, NB)),
        stay(lf[0].T),
        stay(rf[0].T),
        stay(lb[0]),
        stay(rb[0]),
        stay(mom[0]),
        stay(sec[0]),
    )
    upd, nlf, nrf, nmom, nsec = pl.pallas_call(
        finish,
        out_shape=(
            jax.ShapeDtypeStruct((RPD, NB, CPD), BF16),
            jax.ShapeDtypeStruct((CPD, BS), F32),
            jax.ShapeDtypeStruct((CPD, BS), F32),
            jax.ShapeDtypeStruct((BS, BS), BF16),
            jax.ShapeDtypeStruct((BS, BS), F32),
        ),
        in_specs=[vmem] * 6,
        out_specs=[anywhere] * 5,
        scratch_shapes=[pltpu.VMEM((RPD, NB, CPD), BF16), dma((5,))],
        compiler_params=pltpu.CompilerParams(vmem_limit_bytes=16 << 20),
    )(*inner)
    return (jnp.transpose(upd, (1, 0, 2)), nlf.T[None], nrf.T[None], nmom[None], nsec[None])


def solution(mesh):
    block = P("mp", None, None)
    factor = P("mp", None, "dp")
    return jax.shard_map(
        per_device,
        mesh=mesh,
        in_specs=(P("dp", None, "mp", None), P(), P(), factor, factor, block, block, block, block),
        out_specs=(P(None, "mp", "dp"), factor, factor, block, block),
        check_vma=False,
    )
```
